8 devices in a mesh: dp: 1 (over z), ep: 8 (over y, x, core).
Axes of the slice: x: 2, y: 2, z: 1, core: 2. Of those that a mesh axis runs over, the one named last changes fastest.
Arguments:
- x: bfloat16 [16384, 2048], P(('dp', 'ep'))
- route_idx: int32 [16384, 6], P(('dp', 'ep'))
- gates: bfloat16 [16384, 6], P(('dp', 'ep'))
- w1: bfloat16 [72, 2048, 1408], P('ep')
- w3: bfloat16 [72, 2048, 1408], P('ep')
- w2: bfloat16 [72, 1408, 2048], P('ep')
Outputs:
- output: bfloat16 [16384, 2048], P(('dp', 'ep'))
All inputs are finite; a program needn't handle non-finite values.
Results may differ from the reference program's by a relative error of at most 0.00143.
Values are sent between devices in bfloat16 or wider.
A program may use at most 1 GiB of HBM per device.

```python
import jax
import jax.numpy as jnp
from jax import lax

EXPERTS = 64
TOP = 6
D = 2048
FF = 1408
TOKENS_DEV = 2048
EP = 8
BLK = 128

LOC = EXPERTS // EP
SLOTS = LOC + 1
TOKENS = EP * TOKENS_DEV
HOLDERS = [0, (EP // 2 + 1) % EP, (EP // 4 + 2) % EP, (3 * EP // 4 + 3) % EP]


def slot_table(w):
    w = w.astype(jnp.bfloat16).reshape((EP, LOC) + w.shape[1:])
    keep = jnp.zeros((EP, 1, 1), jnp.bfloat16).at[jnp.array(HOLDERS[1:])].set(1.0)
    spare = keep * w[0, 0][None]
    return jnp.concatenate([w, spare[:, None]], axis=1).reshape((EP * SLOTS,) + w.shape[2:])


def setup_inputs(seed: int = 0, part: int = 0) -> dict:
    base = jax.random.fold_in(jax.random.key(seed), part)
    ks = jax.random.split(base, 8)
    kd = jax.random.split(jax.random.fold_in(base, 7), 10)
    kw = jax.random.split(jax.random.key(seed + 1), 3)
    x = jax.random.normal(ks[0], (TOKENS, D), jnp.float32).astype(jnp.bfloat16)
    dens_bits = jax.random.bits(kd[1], (EP, 1), jnp.uint32) >> 8
    dens_cut = jnp.where(dens_bits < 5033165, jnp.uint32(1 << 24), jnp.uint32(838861) + (dens_bits * 2) // 5)
    hot = (jax.random.bits(kd[2], (EP, TOKENS_DEV), jnp.uint32) >> 8) < dens_cut
    off = jax.random.randint(kd[3], (EP, 1, 1), 0, EP)
    step = jnp.where(jax.random.uniform(kd[8], (EP, 1, 1), jnp.float32) < 0.5, 1, EP - 1)
    n = jnp.arange(TOKENS_DEV * TOP).reshape(1, TOKENS_DEV, TOP)
    dev = (off + n * step) % EP
    pop_exp = jax.random.randint(kd[4], (EP, LOC), 0, 13)
    pop_weight = jnp.left_shift(jnp.int32(1), pop_exp).at[0, 0].set(0)
    cum_weight = jnp.cumsum(pop_weight[dev], axis=-1)
    pick_draw = jax.random.randint(kd[5], dev.shape, 0, cum_weight[..., -1])
    local_pick = jnp.sum((pick_draw[..., None] >= cum_weight).astype(jnp.int32), axis=-1)
    cold = dev * LOC + local_pick
    last = jnp.arange(TOP).reshape(1, 1, TOP) == TOP - 1
    e = jnp.where(jnp.logical_and(hot[:, :, None], last), 0, cold).reshape(TOKENS, TOP)
    glogv = jax.random.normal(ks[6], (TOKENS, TOP), jnp.float32) + 0.5 * (e == 0)
    g = jax.nn.softmax(glogv, axis=-1)
    perm = (jnp.arange(TOP)[None, :] + jax.random.randint(kd[7], (TOKENS, 1), 0, TOP)) % TOP
    return dict(
        x=x,
        route_idx=jnp.take_along_axis(e, perm, axis=1).astype(jnp.int32),
        gates=jnp.take_along_axis(g, perm, axis=1).astype(jnp.bfloat16),
        w1=slot_table(jax.random.normal(kw[0], (EXPERTS, D, FF), jnp.float32) * D ** -0.5),
        w3=slot_table(jax.random.normal(kw[1], (EXPERTS, D, FF), jnp.float32) * D ** -0.5),
        w2=slot_table(jax.random.normal(kw[2], (EXPERTS, FF, D), jnp.float32) * FF ** -0.5),
    )


def grouped_ffn(xs, tok, gid, w1, w3, w2):
    n = gid.shape[0]
    d = xs.shape[1]
    g = w1.shape[0]
    nblk = -(-n // BLK) + g
    cnt = jnp.zeros((g + 1,), jnp.int32).at[gid].add(1)[:g]
    padc = (cnt + BLK - 1) // BLK * BLK
    pend = jnp.cumsum(padc)
    pstart = pend - padc
    cstart = jnp.cumsum(cnt) - cnt
    order = jnp.argsort(gid).astype(jnp.int32)
    gs = gid[order]
    gc = jnp.minimum(gs, g - 1)
    pos = jnp.where(gs < g, pstart[gc] + jnp.arange(n, dtype=jnp.int32) - cstart[gc], nblk * BLK)
    src = jnp.full((nblk * BLK,), n, jnp.int32).at[pos].set(order, mode="drop")
    bexp = jnp.minimum(jnp.searchsorted(pend, jnp.arange(nblk, dtype=jnp.int32) * BLK, side="right"), g - 1)
    used = pend[g - 1] // BLK
    xz = jnp.concatenate([xs, jnp.zeros((1, d), xs.dtype)], axis=0)
    tz = jnp.concatenate([tok, jnp.full((1,), xs.shape[0], jnp.int32)], axis=0)

    def body(b, acc):
        xb = xz[tz[lax.dynamic_slice_in_dim(src, b * BLK, BLK)]]
        ex = bexp[b]
        u = jnp.dot(xb, w1[ex], preferred_element_type=jnp.float32)
        v = jnp.dot(xb, w3[ex], preferred_element_type=jnp.float32)
        a = (jax.nn.silu(u) * v).astype(jnp.bfloat16)
        ob = jnp.dot(a, w2[ex], preferred_element_type=jnp.float32).astype(jnp.bfloat16)
        return lax.dynamic_update_slice_in_dim(acc, ob, b * BLK, axis=0)

    acc = lax.fori_loop(0, used, body, jnp.zeros((nblk * BLK, d), jnp.bfloat16))
    return jnp.zeros((n + 1, d), jnp.bfloat16).at[src].set(acc)[:n]


def reference(x, route_idx, gates, w1, w3, w2):
    e = route_idx.reshape(-1)
    slot = (e // LOC) * SLOTS + e % LOC
    tok = jnp.arange(TOKENS * TOP, dtype=jnp.int32) // TOP
    o = grouped_ffn(x, tok, slot, w1, w3, w2).reshape(TOKENS, TOP, D)
    y = jnp.zeros((TOKENS, D), jnp.float32)
    for m in range(TOP):
        y = y + gates[:, m:m + 1].astype(jnp.float32) * o[:, m].astype(jnp.float32)
    return y.astype(jnp.bfloat16)
```

```python
import functools

import jax
import jax.numpy as jnp
from jax import lax
from jax.experimental import pallas as pl
from jax.experimental.pallas import tpu as pltpu
from jax.sharding import PartitionSpec as P


BLK = 128
TM = 256
PIECE = 16
LANES = 128


def relayout_in(src, xf, dst, rows, sub):
    step = 32

    def widen(i, c):
        r = pl.multiple_of(i * step * sub, step * sub)
        xf[pl.ds(r, step * sub), :] = src[pl.ds(r, step * sub), :].astype(jnp.float32)
        return c

    lax.fori_loop(0, rows // step, widen, 0)
    for j in range(sub):
        dst[:, j * LANES:(j + 1) * LANES] = xf[pl.ds(j, rows, stride=sub), :].astype(jnp.bfloat16)


def ffn_kernel(nt, sub, tab, tok, x_hbm, w1, w3, w2, out, xbuf, xf, xb, obuf, gsem, osem):
    i = pl.program_id(0)
    total = tab[3, 0]

    def fetch(t, slot):
        base = tab[1, t]
        nb = (tab[2, t] + PIECE - 1) // PIECE

        def body(b, c):
            for u in range(PIECE):
                row = tok[base + b * PIECE + u]
                pltpu.make_async_copy(
                    x_hbm.at[pl.ds(pl.multiple_of(row * sub, sub), sub)],
                    xbuf.at[slot, pl.ds(pl.multiple_of((b * PIECE + u) * sub, sub), sub)],
                    gsem.at[slot]).start()
            return c

        lax.fori_loop(0, nb, body, 0)

    def out_copies(t, act):
        base = tab[1, t]
        n = tab[2, t]
        full = n // PIECE

        def big(b, c):
            act(pltpu.make_async_copy(
                obuf.at[pl.ds(pl.multiple_of(b * PIECE * sub, PIECE * sub), PIECE * sub)],
                out.at[pl.ds(pl.multiple_of((base + b * PIECE) * sub, sub), PIECE * sub)], osem))
            return c

        def small(b, c):
            act(pltpu.make_async_copy(
                obuf.at[pl.ds(pl.multiple_of(b * sub, sub), sub)],
                out.at[pl.ds(pl.multiple_of((base + b) * sub, sub), sub)], osem))
            return c

        lax.fori_loop(0, full, big, 0)
        lax.fori_loop(full * PIECE, n, small, 0)

    @pl.when(i == 0)
    def _():
        fetch(0, 0)

    @pl.when(i + 1 < total)
    def _():
        fetch(i + 1, (i + 1) % 2)

    @pl.when(i < total)
    def _():
        slot = i % 2

        def wait(b, c):
            pltpu.make_async_copy(
                x_hbm.at[pl.ds(0, PIECE * sub)], xbuf.at[slot, pl.ds(0, PIECE * sub)], gsem.at[slot]).wait()
            return c

        lax.fori_loop(0, (tab[2, i] + PIECE - 1) // PIECE, wait, 0)
        relayout_in(xbuf.at[slot], xf, xb, TM, sub)
        u = jnp.dot(xb[...], w1[0], preferred_element_type=jnp.float32)
        v = jnp.dot(xb[...], w3[0], preferred_element_type=jnp.float32)
        a = (u * jax.nn.sigmoid(u) * v).astype(jnp.bfloat16)

        @pl.when(i > 0)
        def _():
            out_copies(i - 1, lambda c: c.wait())

        half = sub // 2
        for h in range(2):
            o = jnp.dot(a, w2[0, :, h * half * LANES:(h + 1) * half * LANES], preferred_element_type=jnp.float32)
            for j in range(half):
                xf[pl.ds(h * half + j, TM, stride=sub), :] = o[:, j * LANES:(j + 1) * LANES]

        def narrow(b, c):
            r = pl.multiple_of(b * 32 * sub, 32 * sub)
            obuf[pl.ds(r, 32 * sub), :] = xf[pl.ds(r, 32 * sub), :].astype(jnp.bfloat16)
            return c

        lax.fori_loop(0, TM // 32, narrow, 0)
        out_copies(i, lambda c: c.start())

    @pl.when(jnp.logical_and(i == nt - 1, total > 0))
    def _():
        out_copies(total - 1, lambda c: c.wait())


def ffn(tab, tok, x3, w1, w3, w2, cap):
    nt = tab.shape[1]
    d, f = w1.shape[1:]
    sub = d // LANES
    wspec = lambda shape: pl.BlockSpec((1,) + shape, lambda i, tab, tok: (tab[0, i], 0, 0))
    return pl.pallas_call(
        functools.partial(ffn_kernel, nt, sub),
        out_shape=jax.ShapeDtypeStruct((cap * sub, LANES), jnp.bfloat16),
        grid_spec=pltpu.PrefetchScalarGridSpec(
            num_scalar_prefetch=2,
            grid=(nt,),
            in_specs=[pl.BlockSpec(memory_space=pl.ANY), wspec((d, f)), wspec((d, f)), wspec((f, d))],
            out_specs=pl.BlockSpec(memory_space=pl.ANY),
            scratch_shapes=[
                pltpu.VMEM((2, TM * sub, LANES), jnp.bfloat16),
                pltpu.VMEM((TM * sub, LANES), jnp.float32),
                pltpu.VMEM((TM, d), jnp.bfloat16),
                pltpu.VMEM((TM * sub, LANES), jnp.bfloat16),
                pltpu.SemaphoreType.DMA((2,)),
                pltpu.SemaphoreType.DMA,
            ]),
        compiler_params=pltpu.CompilerParams(
            dimension_semantics=("arbitrary",), vmem_limit_bytes=60 * 1024 * 1024),
        cost_estimate=pl.CostEstimate(flops=6 * cap * d * f, bytes_accessed=6 * 8 * d * f, transcendentals=cap * f),
        name="expert_ffn",
    )(tab, tok, x3, w1, w3, w2)


RB = 256


def combine_kernel(nbs, sub, first, final, meta, tok_ref, gate_ref, *refs):
    nsrc = len(nbs)
    srcs = refs[:nsrc]
    rest = refs[nsrc:]
    if not first:
        acc_in, rest = rest[0], rest[1:]
    out, acc, buf, xf, xb, sem, asem = rest[:7]
    td, d = acc.shape
    steps = [(q, b) for q in range(nsrc) for b in range(nbs[q])]
    total = len(steps)
    i = pl.program_id(0)
    off = [sum(nbs[:q]) for q in range(nsrc)]
    rows = RB * sub

    def each_source(t, fn):
        for q in range(nsrc):
            @pl.when(jnp.logical_and(t >= off[q], t < off[q] + nbs[q]))
            def _(q=q):
                b = t - off[q]
                fn(srcs[q].at[pl.ds(pl.multiple_of(b * rows, rows), rows)])

    def live(t):
        return meta[t] > 0

    @pl.when(i == 0)
    def _():
        if first:
            acc[...] = jnp.zeros_like(acc)
        else:
            cp = pltpu.make_async_copy(acc_in, acc, asem)
            cp.start()

        @pl.when(live(0))
        def _():
            each_source(0, lambda r: pltpu.make_async_copy(r, buf.at[0], sem.at[0]).start())

        if not first:
            cp.wait()

    @pl.when(i + 1 < total)
    def _():
        @pl.when(live(i + 1))
        def _():
            each_source(i + 1, lambda r: pltpu.make_async_copy(r, buf.at[(i + 1) % 2], sem.at[(i + 1) % 2]).start())

    @pl.when(live(i))
    def _():
        pltpu.make_async_copy(srcs[0].at[pl.ds(0, rows)], buf.at[i % 2], sem.at[i % 2]).wait()
        relayout_in(buf.at[i % 2], xf, xb, RB, sub)
        n = meta[i]

        @pl.when(n < RB)
        def _():
            keep = lax.broadcasted_iota(jnp.int32, (RB, LANES), 0) < n
            for j in range(sub):
                cur = xb[:, j * LANES:(j + 1) * LANES].astype(jnp.float32)
                xb[:, j * LANES:(j + 1) * LANES] = jnp.where(keep, cur, 0.0).astype(jnp.bfloat16)

        tb = 256

        def tokens(c, z):
            r = pl.multiple_of(c * tb, tb)
            ids = lax.broadcasted_iota(jnp.int32, (tb, RB), 0) + r
            g = jnp.where(ids == tok_ref[0], gate_ref[0], 0.0).astype(jnp.bfloat16)
            acc[pl.ds(r, tb), :] += jnp.dot(g, xb[...], preferred_element_type=jnp.float32)
            return z

        lax.fori_loop(0, td // tb, tokens, 0)

    @pl.when(i == total - 1)
    def _():
        if final:
            ob = rest[7]
            cb = 256
            for c in range(td // cb):
                if c >= 2:
                    pltpu.make_async_copy(ob.at[c % 2], out.at[pl.ds((c - 2) * cb, cb)], sem.at[c % 2]).wait()
                ob[c % 2] = acc[c * cb:(c + 1) * cb, :].astype(jnp.bfloat16)
                pltpu.make_async_copy(ob.at[c % 2], out.at[pl.ds(c * cb, cb)], sem.at[c % 2]).start()
            for c in (td // cb - 2, td // cb - 1):
                pltpu.make_async_copy(ob.at[c % 2], out.at[pl.ds(c * cb, cb)], sem.at[c % 2]).wait()
        else:
            cp = pltpu.make_async_copy(acc, out, asem)
            cp.start()
            cp.wait()


def combine(acc, srcs, toks, gates, lens, td, d, final):
    sub = d // LANES
    nbs = [s.shape[0] // (RB * sub) for s in srcs]
    first = acc is None
    meta = jnp.concatenate([jnp.clip(n - jnp.arange(nb, dtype=jnp.int32) * RB, 0, RB) for n, nb in zip(lens, nbs)])
    total = sum(nbs)
    tokv = jnp.concatenate(toks).reshape(total, 1, RB)
    gatev = jnp.concatenate(gates).reshape(total, 1, RB)
    vspec = pl.BlockSpec((1, 1, RB), lambda i, m: (i, 0, 0))
    scratch = [
        pltpu.VMEM((td, d), jnp.float32),
        pltpu.VMEM((2, RB * sub, LANES), jnp.bfloat16),
        pltpu.VMEM((RB * sub, LANES), jnp.float32),
        pltpu.VMEM((RB, d), jnp.bfloat16),
        pltpu.SemaphoreType.DMA((2,)),
        pltpu.SemaphoreType.DMA,
    ]
    if final:
        scratch.append(pltpu.VMEM((2, 256, d), jnp.bfloat16))
    extra = [] if first else [acc]
    return pl.pallas_call(
        functools.partial(combine_kernel, nbs, sub, first, final),
        out_shape=jax.ShapeDtypeStruct((td, d), jnp.bfloat16 if final else jnp.float32),
        grid_spec=pltpu.PrefetchScalarGridSpec(
            num_scalar_prefetch=1,
            grid=(total,),
            in_specs=[vspec, vspec] + [pl.BlockSpec(memory_space=pl.ANY)] * (len(srcs) + len(extra)),
            out_specs=pl.BlockSpec(memory_space=pl.ANY),
            scratch_shapes=scratch),
        compiler_params=pltpu.CompilerParams(
            dimension_semantics=("arbitrary",), vmem_limit_bytes=48 * 1024 * 1024),
        cost_estimate=pl.CostEstimate(flops=2 * total * RB * td * d, bytes_accessed=total * RB * d * 2, transcendentals=0),
        name="combine",
    )(meta, tokv, gatev, *srcs, *extra)


def plan(ridx, gates, near, ep, loc):
    td, k = ridx.shape
    n = td * k
    ne = ep * loc
    ns = loc + 1
    nb = n // BLK
    e = ridx.reshape(nb, BLK)
    oh = e[:, :, None] == jnp.arange(ne, dtype=jnp.int32)
    ohb = oh.astype(jnp.bfloat16)
    tri = (jnp.arange(BLK)[:, None] > jnp.arange(BLK)[None, :]).astype(jnp.bfloat16)
    inb = jnp.einsum("ij,bjg->big", tri, ohb, preferred_element_type=jnp.float32)
    tot = jnp.sum(ohb.astype(jnp.float32), axis=1)
    low = (jnp.arange(nb)[:, None] > jnp.arange(nb)[None, :]).astype(jnp.bfloat16)
    before = jnp.dot(low, tot.astype(jnp.bfloat16), preferred_element_type=jnp.float32)
    cnt = (before[-1] + tot[-1]).astype(jnp.int32)
    h = cnt[0]
    cold = cnt.at[0].set(0).reshape(ep, loc)
    per = jnp.sum(cold, axis=1)
    h0 = jnp.clip((per[near + 1] + h - per[near]) // 2, 0, h)
    dev = jnp.arange(ep, dtype=jnp.int32)
    hotc = jnp.where(dev == near, h0, 0) + jnp.where(dev == near + 1, h - h0, 0)
    groups = jnp.concatenate([cold, hotc[:, None]], axis=1).reshape(-1)
    ends = jnp.cumsum(groups)
    starts = ends - groups
    st = starts.reshape(ep, ns)
    off = st[:, :loc].reshape(-1).at[0].set(0).astype(jnp.float32)
    r = jnp.sum(jnp.where(oh, inb + (before + off)[:, None, :], 0.0), axis=2).astype(jnp.int32)
    hot = jnp.where(r < h0, st[near, loc] + r, st[near + 1, loc] + r - h0)
    pos = jnp.where(e == 0, hot, r).reshape(n)
    hi = (pos[:, None] // BLK == jnp.arange(nb, dtype=jnp.int32)).astype(jnp.bfloat16)
    lo = pos[:, None] % BLK == jnp.arange(BLK, dtype=jnp.int32)
    t = jnp.arange(n, dtype=jnp.int32) // k
    vals = [(t // BLK).astype(jnp.bfloat16), (t % BLK).astype(jnp.bfloat16), gates.reshape(n)]
    rhs = jnp.concatenate([jnp.where(lo, v[:, None], jnp.zeros((), jnp.bfloat16)) for v in vals], axis=1)
    m = jnp.einsum("nh,nl->hl", hi, rhs, preferred_element_type=jnp.float32)
    tok = (m[:, :BLK] * BLK + m[:, BLK:2 * BLK]).astype(jnp.int32).reshape(n)
    return tok, m[:, 2 * BLK:].reshape(n), starts, groups


def tile_table(counts, slots, nt):
    tiles = (counts + TM - 1) // TM
    tend = jnp.cumsum(tiles)
    rstart = jnp.cumsum(counts) - counts
    total = tend[-1]
    i = jnp.arange(nt, dtype=jnp.int32)
    ic = jnp.minimum(i, jnp.maximum(total - 1, 0))
    sel = jnp.sum((ic[:, None] >= tend[None, :]).astype(jnp.int32), axis=1)
    one = sel[:, None] == jnp.arange(counts.shape[0], dtype=jnp.int32)
    pick = lambda v: jnp.sum(jnp.where(one, v, 0), axis=1)
    within = (ic - pick(tend - tiles)) * TM
    rows = jnp.where(i < total, jnp.minimum(pick(counts) - within, TM), 0)
    return jnp.stack([pick(slots), pick(rstart) + within, rows, jnp.broadcast_to(total, (nt,))]).astype(jnp.int32)


def solution(mesh):
    p = mesh.shape["ep"]

    def local(x, ridx, gates, w1, w3, w2):
        td, d = x.shape
        k = ridx.shape[1]
        ns = w1.shape[0]
        loc = ns - 1
        sub = d // LANES
        n = td * k
        capc = n // p
        caph = capc + td // 2
        caps = [caph] * 4 + [capc] * 4
        me = lax.axis_index("ep")
        swap = lambda v, b: lax.ppermute(v, "ep", [(q, q ^ b) for q in range(p)])

        x3 = x.reshape(td * sub, LANES)
        blk = {0: x3}
        blk[1] = swap(x3, 1)
        blk[2] = swap(x3, 2)
        blk[4] = swap(x3, 4)
        blk[3] = swap(blk[2], 1)
        blk[6] = swap(blk[2], 4)
        blk[5] = swap(blk[4], 1)
        blk[7] = swap(blk[6], 1)

        near = me // 4 * 4
        tok, gate, starts, groups = plan(ridx, gates, near, p, loc)
        info = jnp.concatenate([tok, jnp.zeros((caph,), jnp.int32), starts, groups])
        info = jnp.pad(info, (0, -info.shape[0] % LANES))
        every = lax.all_gather(info, "ep")
        slots = jnp.arange(ns, dtype=jnp.int32)
        slots = jnp.where(jnp.logical_and(slots == loc, me == 0), 0, slots)

        gatep = jnp.concatenate([gate, jnp.zeros((caph,), jnp.float32)])
        tokp = info[:n + caph]
        outs, toks, gts, lens = {}, {}, {}, {}
        for j in (0, 1, 2, 3, 4, 5, 6, 7):
            cap = caps[j]
            row = lax.dynamic_index_in_dim(every, me ^ j, 0, keepdims=False)
            first = n + caph + me * ns
            start = lax.dynamic_index_in_dim(row, first, 0, keepdims=False)
            counts = lax.dynamic_slice_in_dim(row, first + p * ns, ns)
            seg = lax.dynamic_slice_in_dim(row, start, cap + PIECE)
            tab = tile_table(counts, slots, cap // TM + ns)
            o = ffn(tab, seg, blk[j], w1, w3, w2, cap)
            outs[j] = swap(o, j) if j else o
            b = me ^ j
            mine = lax.dynamic_index_in_dim(starts, b * ns, 0, keepdims=False)
            lens[j] = jnp.sum(lax.dynamic_slice_in_dim(groups, b * ns, ns))
            toks[j] = lax.dynamic_slice_in_dim(tokp, mine, cap)
            gts[j] = lax.dynamic_slice_in_dim(gatep, mine, cap)
        acc = None
        for part in ((0, 1, 2, 3), (4, 5), (6, 7)):
            pick = lambda m: [m[j] for j in part]
            acc = combine(acc, pick(outs), pick(toks), pick(gts), pick(lens), td, d, part[-1] == 7)
        return acc

    spec_t = P(("dp", "ep"), None)
    spec_w = P("ep", None, None)
    return jax.shard_map(local, mesh=mesh, in_specs=(spec_t, spec_t, spec_t, spec_w, spec_w, spec_w), out_specs=spec_t, check_vma=False)
```

```python
import functools

import jax
import jax.numpy as jnp
from jax import lax
from jax.experimental import pallas as pl
from jax.experimental.pallas import tpu as pltpu
from jax.sharding import PartitionSpec as P


BLK = 128
TM = 256
PIECE = 16
TAIL = 128
COLS = 512
OSUB = 4
LANES = 128
ORDER = (0, 2, 3, 4, 5, 6, 7, 1)
PARTS = ((0, 1, 2), (3, 4), (5, 6), (7,))


def relayout_in(src, xf, dst, rows, sub):
    step = 32

    def widen(i, c):
        r = pl.multiple_of(i * step * sub, step * sub)
        xf[pl.ds(r, step * sub), :] = src[pl.ds(r, step * sub), :].astype(jnp.float32)
        return c

    lax.fori_loop(0, rows // step, widen, 0)
    for j in range(sub):
        dst[:rows, j * LANES:(j + 1) * LANES] = xf[pl.ds(j, rows, stride=sub), :].astype(jnp.bfloat16)


def ffn_kernel(nt, sub, tab, tok, x_hbm, w1, w3, w2, out, xbuf, xf, xb, ab, obuf, gsem, osem):
    i = pl.program_id(0)
    total = tab[3, 0]

    def fetch(t, slot):
        base = tab[1, t]
        nb = (tab[2, t] + PIECE - 1) // PIECE

        def body(b, c):
            for u in range(PIECE):
                row = tok[base + b * PIECE + u]
                pltpu.make_async_copy(
                    x_hbm.at[pl.ds(pl.multiple_of(row * sub, sub), sub)],
                    xbuf.at[slot, pl.ds(pl.multiple_of((b * PIECE + u) * sub, sub), sub)],
                    gsem.at[slot]).start()
            return c

        lax.fori_loop(0, nb, body, 0)

    def out_copies(t, act):
        base = tab[1, t]
        n = tab[2, t]
        full = n // PIECE

        def big(b, c):
            act(pltpu.make_async_copy(
                obuf.at[pl.ds(pl.multiple_of(b * PIECE * sub, PIECE * sub), PIECE * sub)],
                out.at[pl.ds(pl.multiple_of((base + b * PIECE) * sub, sub), PIECE * sub)], osem))
            return c

        def small(b, c):
            act(pltpu.make_async_copy(
                obuf.at[pl.ds(pl.multiple_of(b * sub, sub), sub)],
                out.at[pl.ds(pl.multiple_of((base + b) * sub, sub), sub)], osem))
            return c

        lax.fori_loop(0, full, big, 0)
        lax.fori_loop(full * PIECE, n, small, 0)

    @pl.when(i == 0)
    def _():
        fetch(0, 0)

    @pl.when(i + 1 < total)
    def _():
        fetch(i + 1, (i + 1) % 2)

    @pl.when(i < total)
    def _():
        slot = i % 2

        def wait(b, c):
            pltpu.make_async_copy(
                x_hbm.at[pl.ds(0, PIECE * sub)], xbuf.at[slot, pl.ds(0, PIECE * sub)], gsem.at[slot]).wait()
            return c

        lax.fori_loop(0, (tab[2, i] + PIECE - 1) // PIECE, wait, 0)

        def compute(m):
            relayout_in(xbuf.at[slot], xf, xb, m, sub)
            x = xb[:m, :]
            f = w1.shape[2]
            for c in range(0, f, COLS):
                hi = min(c + COLS, f)
                u = jnp.dot(x, w1[0, :, c:hi], preferred_element_type=jnp.float32)
                v = jnp.dot(x, w3[0, :, c:hi], preferred_element_type=jnp.float32)
                ab[:m, c:hi] = (u * jax.nn.sigmoid(u) * v).astype(jnp.bfloat16)
            a = ab[:m, :]
            for h in range(0, sub, OSUB):
                o = jnp.dot(a, w2[0, :, h * LANES:(h + OSUB) * LANES], preferred_element_type=jnp.float32)
                for j in range(OSUB):
                    xf[pl.ds(h + j, m, stride=sub), :] = o[:, j * LANES:(j + 1) * LANES]

            @pl.when(i > 0)
            def _():
                out_copies(i - 1, lambda c: c.wait())

            def narrow(b, c):
                r = pl.multiple_of(b * 32 * sub, 32 * sub)
                obuf[pl.ds(r, 32 * sub), :] = xf[pl.ds(r, 32 * sub), :].astype(jnp.bfloat16)
                return c

            lax.fori_loop(0, m // 32, narrow, 0)

        if TAIL:
            @pl.when(tab[2, i] > TAIL)
            def _():
                compute(TM)

            @pl.when(tab[2, i] <= TAIL)
            def _():
                compute(TAIL)
        else:
            compute(TM)
        out_copies(i, lambda c: c.start())

    @pl.when(jnp.logical_and(i == nt - 1, total > 0))
    def _():
        out_copies(total - 1, lambda c: c.wait())


def ffn(tab, tok, x3, w1, w3, w2, cap):
    nt = tab.shape[1]
    d, f = w1.shape[1:]
    sub = d // LANES
    wspec = lambda shape: pl.BlockSpec((1,) + shape, lambda i, tab, tok: (tab[0, i], 0, 0))
    return pl.pallas_call(
        functools.partial(ffn_kernel, nt, sub),
        out_shape=jax.ShapeDtypeStruct((cap * sub, LANES), jnp.bfloat16),
        grid_spec=pltpu.PrefetchScalarGridSpec(
            num_scalar_prefetch=2,
            grid=(nt,),
            in_specs=[pl.BlockSpec(memory_space=pl.ANY), wspec((d, f)), wspec((d, f)), wspec((f, d))],
            out_specs=pl.BlockSpec(memory_space=pl.ANY),
            scratch_shapes=[
                pltpu.VMEM((2, TM * sub, LANES), jnp.bfloat16),
                pltpu.VMEM((TM * sub, LANES), jnp.float32),
                pltpu.VMEM((TM, d), jnp.bfloat16),
                pltpu.VMEM((TM, f), jnp.bfloat16),
                pltpu.VMEM((TM * sub, LANES), jnp.bfloat16),
                pltpu.SemaphoreType.DMA((2,)),
                pltpu.SemaphoreType.DMA,
            ]),
        compiler_params=pltpu.CompilerParams(
            dimension_semantics=("arbitrary",), vmem_limit_bytes=60 * 1024 * 1024),
        cost_estimate=pl.CostEstimate(flops=6 * cap * d * f, bytes_accessed=6 * 8 * d * f, transcendentals=cap * f),
        name="expert_ffn",
    )(tab, tok, x3, w1, w3, w2)


RB = 512


def combine_kernel(nbs, sub, first, final, meta, tok_ref, gate_ref, *refs):
    nsrc = len(nbs)
    srcs = refs[:nsrc]
    rest = refs[nsrc:]
    if not first:
        acc_in, rest = rest[0], rest[1:]
    out, acc, buf, xf, xb, sem, asem = rest[:7]
    td, d = acc.shape
    steps = [(q, b) for q in range(nsrc) for b in range(nbs[q])]
    total = len(steps)
    i = pl.program_id(0)
    off = [sum(nbs[:q]) for q in range(nsrc)]
    rows = RB * sub

    def each_source(t, fn):
        for q in range(nsrc):
            @pl.when(jnp.logical_and(t >= off[q], t < off[q] + nbs[q]))
            def _(q=q):
                b = t - off[q]
                fn(srcs[q].at[pl.ds(pl.multiple_of(b * rows, rows), rows)])

    def live(t):
        return meta[t] > 0

    @pl.when(i == 0)
    def _():
        if first:
            acc[...] = jnp.zeros_like(acc)
        else:
            cp = pltpu.make_async_copy(acc_in, acc, asem)
            cp.start()

        @pl.when(live(0))
        def _():
            each_source(0, lambda r: pltpu.make_async_copy(r, buf.at[0], sem.at[0]).start())

        if not first:
            cp.wait()

    @pl.when(i + 1 < total)
    def _():
        @pl.when(live(i + 1))
        def _():
            each_source(i + 1, lambda r: pltpu.make_async_copy(r, buf.at[(i + 1) % 2], sem.at[(i + 1) % 2]).start())

    @pl.when(live(i))
    def _():
        pltpu.make_async_copy(srcs[0].at[pl.ds(0, rows)], buf.at[i % 2], sem.at[i % 2]).wait()
        relayout_in(buf.at[i % 2], xf, xb, RB, sub)
        n = meta[i]

        @pl.when(n < RB)
        def _():
            keep = lax.broadcasted_iota(jnp.int32, (RB, LANES), 0) < n
            for j in range(sub):
                cur = xb[:, j * LANES:(j + 1) * LANES].astype(jnp.float32)
                xb[:, j * LANES:(j + 1) * LANES] = jnp.where(keep, cur, 0.0).astype(jnp.bfloat16)

        tb = 256

        def tokens(c, z):
            r = pl.multiple_of(c * tb, tb)
            ids = lax.broadcasted_iota(jnp.int32, (tb, RB), 0) + r
            g = jnp.where(ids == tok_ref[0], gate_ref[0], 0.0).astype(jnp.bfloat16)
            acc[pl.ds(r, tb), :] += jnp.dot(g, xb[...], preferred_element_type=jnp.float32)
            return z

        lax.fori_loop(0, td // tb, tokens, 0)

    @pl.when(i == total - 1)
    def _():
        if final:
            ob = rest[7]
            cb = 256
            for c in range(td // cb):
                if c >= 2:
                    pltpu.make_async_copy(ob.at[c % 2], out.at[pl.ds((c - 2) * cb, cb)], sem.at[c % 2]).wait()
                ob[c % 2] = acc[c * cb:(c + 1) * cb, :].astype(jnp.bfloat16)
                pltpu.make_async_copy(ob.at[c % 2], out.at[pl.ds(c * cb, cb)], sem.at[c % 2]).start()
            for c in (td // cb - 2, td // cb - 1):
                pltpu.make_async_copy(ob.at[c % 2], out.at[pl.ds(c * cb, cb)], sem.at[c % 2]).wait()
        else:
            cp = pltpu.make_async_copy(acc, out, asem)
            cp.start()
            cp.wait()


def combine(acc, srcs, toks, gates, lens, td, d, final):
    sub = d // LANES
    nbs = [s.shape[0] // (RB * sub) for s in srcs]
    first = acc is None
    meta = jnp.concatenate([jnp.clip(n - jnp.arange(nb, dtype=jnp.int32) * RB, 0, RB) for n, nb in zip(lens, nbs)])
    total = sum(nbs)
    tokv = jnp.concatenate(toks).reshape(total, 1, RB)
    gatev = jnp.concatenate(gates).reshape(total, 1, RB)
    vspec = pl.BlockSpec((1, 1, RB), lambda i, m: (i, 0, 0))
    scratch = [
        pltpu.VMEM((td, d), jnp.float32),
        pltpu.VMEM((2, RB * sub, LANES), jnp.bfloat16),
        pltpu.VMEM((RB * sub, LANES), jnp.float32),
        pltpu.VMEM((RB, d), jnp.bfloat16),
        pltpu.SemaphoreType.DMA((2,)),
        pltpu.SemaphoreType.DMA,
    ]
    if final:
        scratch.append(pltpu.VMEM((2, 256, d), jnp.bfloat16))
    extra = [] if first else [acc]
    return pl.pallas_call(
        functools.partial(combine_kernel, nbs, sub, first, final),
        out_shape=jax.ShapeDtypeStruct((td, d), jnp.bfloat16 if final else jnp.float32),
        grid_spec=pltpu.PrefetchScalarGridSpec(
            num_scalar_prefetch=1,
            grid=(total,),
            in_specs=[vspec, vspec] + [pl.BlockSpec(memory_space=pl.ANY)] * (len(srcs) + len(extra)),
            out_specs=pl.BlockSpec(memory_space=pl.ANY),
            scratch_shapes=scratch),
        compiler_params=pltpu.CompilerParams(
            dimension_semantics=("arbitrary",), vmem_limit_bytes=48 * 1024 * 1024),
        cost_estimate=pl.CostEstimate(flops=2 * total * RB * td * d, bytes_accessed=total * RB * d * 2, transcendentals=0),
        name="combine",
    )(meta, tokv, gatev, *srcs, *extra)


def plan(ridx, gates, near, ep, loc):
    td, k = ridx.shape
    n = td * k
    ne = ep * loc
    ns = loc + 1
    nb = n // BLK
    e = ridx.reshape(nb, BLK)
    oh = e[:, :, None] == jnp.arange(ne, dtype=jnp.int32)
    ohb = oh.astype(jnp.bfloat16)
    tri = (jnp.arange(BLK)[:, None] > jnp.arange(BLK)[None, :]).astype(jnp.bfloat16)
    inb = jnp.einsum("ij,bjg->big", tri, ohb, preferred_element_type=jnp.float32)
    tot = jnp.sum(ohb.astype(jnp.float32), axis=1)
    low = (jnp.arange(nb)[:, None] > jnp.arange(nb)[None, :]).astype(jnp.bfloat16)
    before = jnp.dot(low, tot.astype(jnp.bfloat16), preferred_element_type=jnp.float32)
    cnt = (before[-1] + tot[-1]).astype(jnp.int32)
    h = cnt[0]
    cold = cnt.at[0].set(0).reshape(ep, loc)
    per = jnp.sum(cold, axis=1)
    h0 = jnp.clip((per[near + 1] + h - per[near]) // 2, 0, h)
    dev = jnp.arange(ep, dtype=jnp.int32)
    hotc = jnp.where(dev == near, h0, 0) + jnp.where(dev == near + 1, h - h0, 0)
    groups = jnp.concatenate([cold, hotc[:, None]], axis=1).reshape(-1)
    starts = prefix(groups) - groups
    st = starts.reshape(ep, ns)
    off = st[:, :loc].reshape(-1).at[0].set(0).astype(jnp.float32)
    r = jnp.sum(jnp.where(oh, inb + (before + off)[:, None, :], 0.0), axis=2).astype(jnp.int32)
    hot = jnp.where(r < h0, st[near, loc] + r, st[near + 1, loc] + r - h0)
    pos = jnp.where(e == 0, hot, r).reshape(n)
    hi = (pos[:, None] // BLK == jnp.arange(nb, dtype=jnp.int32)).astype(jnp.bfloat16)
    lo = pos[:, None] % BLK == jnp.arange(BLK, dtype=jnp.int32)
    t = jnp.arange(n, dtype=jnp.int32) // k
    vals = [(t // BLK).astype(jnp.bfloat16), (t % BLK).astype(jnp.bfloat16), gates.reshape(n)]
    rhs = jnp.concatenate([jnp.where(lo, v[:, None], jnp.zeros((), jnp.bfloat16)) for v in vals], axis=1)
    m = jnp.einsum("nh,nl->hl", hi, rhs, preferred_element_type=jnp.float32)
    tok = (m[:, :BLK] * BLK + m[:, BLK:2 * BLK]).astype(jnp.int32).reshape(n)
    return tok, m[:, 2 * BLK:].reshape(n), starts, groups


def prefix(v):
    m = v.shape[-1]
    upto = jnp.arange(m)[:, None] <= jnp.arange(m)[None, :]
    return jnp.sum(jnp.where(upto, v[..., :, None], 0), axis=-2)


def tile_tables(counts, nt):
    ep, ns = counts.shape
    tiles = (counts + TM - 1) // TM
    tend = prefix(tiles)
    rstart = prefix(counts) - counts
    total = tend[:, -1:]
    slot = jnp.arange(ns, dtype=jnp.int32)[None, :]
    owner = jnp.arange(ep)[:, None] == 0
    slots = jnp.where(jnp.logical_and(slot == ns - 1, owner), 0, slot)
    i = jnp.arange(nt, dtype=jnp.int32)[None, :]
    ic = jnp.minimum(i, jnp.maximum(total - 1, 0))
    sel = jnp.sum((ic[:, :, None] >= tend[:, None, :]).astype(jnp.int32), axis=2)
    one = sel[:, :, None] == slot[:, None, :]
    pick = lambda v: jnp.sum(jnp.where(one, v[:, None, :], 0), axis=2)
    within = (ic - pick(tend - tiles)) * TM
    rows = jnp.where(i < total, jnp.minimum(pick(counts) - within, TM), 0)
    tab = jnp.stack([pick(slots), pick(rstart) + within, rows, jnp.broadcast_to(total, (ep, nt))], axis=1)
    return tab.astype(jnp.int32)


def solution(mesh):
    p = mesh.shape["ep"]

    def local(x, ridx, gates, w1, w3, w2):
        td, d = x.shape
        k = ridx.shape[1]
        ns = w1.shape[0]
        loc = ns - 1
        sub = d // LANES
        n = td * k
        capc = n // p
        caph = capc + td // 2
        caps = [caph] * 4 + [capc] * 4
        me = lax.axis_index("ep")
        swap = lambda v, b: lax.ppermute(v, "ep", [(q, q ^ b) for q in range(p)])

        near = me // 4 * 4
        nt = caph // TM + ns
        tok, gate, starts, groups = plan(ridx, gates, near, p, loc)
        tabs = tile_tables(groups.reshape(p, ns), nt)
        recs = jnp.concatenate([starts.reshape(p, ns)[:, :1], tabs.reshape(p, 4 * nt)], axis=1)
        recs = jnp.pad(recs, ((0, 0), (0, LANES - recs.shape[1])))
        pad = -(-(caph + PIECE) // LANES) * LANES
        tokp = jnp.concatenate([tok, jnp.zeros((pad,), jnp.int32)])
        every = lax.all_gather(jnp.concatenate([tokp, recs.reshape(-1)]), "ep")

        x3 = x.reshape(td * sub, LANES)
        blk = {0: x3, 1: swap(x3, 1)}
        x3, every = lax.optimization_barrier((x3, every))
        blk[2] = swap(x3, 2)
        blk[4] = swap(x3, 4)
        blk[3] = swap(blk[2], 1)
        blk[6] = swap(blk[2], 4)
        blk[5] = swap(blk[4], 1)
        blk[7] = swap(blk[6], 1)

        rec = lax.dynamic_slice_in_dim(every, n + pad + me * LANES, LANES, axis=1)
        dev = jnp.arange(p, dtype=jnp.int32)
        rel = (me ^ dev)[:, None] == dev[None, :]
        rec = jnp.sum(jnp.where(rel[:, :, None], rec[None, :, :], 0), axis=1)
        gatep = jnp.concatenate([gate, jnp.zeros((pad,), jnp.float32)])
        per = jnp.sum(groups.reshape(p, ns), axis=1)
        outs, toks, gts, lens = {}, {}, {}, {}
        for j in ORDER:
            cap = caps[j]
            seg = lax.dynamic_slice(every, (me ^ j, rec[j, 0]), (1, cap + PIECE)).reshape(cap + PIECE)
            tab = rec[j, 1:1 + 4 * nt].reshape(4, nt)[:, :cap // TM + ns]
            o = ffn(tab, seg, blk[j], w1, w3, w2, cap)
            outs[j] = swap(o, j) if j else o
            mine = lax.dynamic_index_in_dim(starts, (me ^ j) * ns, 0, keepdims=False)
            lens[j] = lax.dynamic_index_in_dim(per, me ^ j, 0, keepdims=False)
            toks[j] = lax.dynamic_slice_in_dim(tokp, mine, cap)
            gts[j] = lax.dynamic_slice_in_dim(gatep, mine, cap)
        acc = None
        for part in PARTS:
            pick = lambda m: [m[j] for j in part]
            acc = combine(acc, pick(outs), pick(toks), pick(gts), pick(lens), td, d, part is PARTS[-1])
        return acc

    spec_t = P(("dp", "ep"), None)
    spec_w = P("ep", None, None)
    return jax.shard_map(local, mesh=mesh, in_specs=(spec_t, spec_t, spec_t, spec_w, spec_w, spec_w), out_specs=spec_t, check_vma=False)
```

```python
import functools

import jax
import jax.numpy as jnp
from jax import lax
from jax.experimental import pallas as pl
from jax.experimental.pallas import tpu as pltpu
from jax.sharding import PartitionSpec as P


BLK = 128
TM = 256
PIECE = 16
TAIL = 128
COLS = 512
OSUB = 4
LANES = 128
HOT = 8
ORDER = (0, 2, 4, 3, 5, 6, 7, 1, HOT)
PARTS = ((0, 1, 2, 4, HOT), (3, 5), (6,), (7,))


def relayout_in(src, xf, dst, rows, sub):
    step = 32

    def widen(i, c):
        r = pl.multiple_of(i * step * sub, step * sub)
        xf[pl.ds(r, step * sub), :] = src[pl.ds(r, step * sub), :].astype(jnp.float32)
        return c

    lax.fori_loop(0, rows // step, widen, 0)
    for j in range(sub):
        dst[:rows, j * LANES:(j + 1) * LANES] = xf[pl.ds(j, rows, stride=sub), :].astype(jnp.bfloat16)


def ffn_kernel(nt, sub, tab, tok, x_hbm, w1, w3, w2, out, xbuf, xf, xb, ab, obuf, gsem, osem):
    i = pl.program_id(0)
    total = tab[3, 0]

    def fetch(t, slot):
        base = tab[1, t]
        nb = (tab[2, t] + PIECE - 1) // PIECE

        def body(b, c):
            for u in range(PIECE):
                row = tok[base + b * PIECE + u]
                pltpu.make_async_copy(
                    x_hbm.at[pl.ds(pl.multiple_of(row * sub, sub), sub)],
                    xbuf.at[slot, pl.ds(pl.multiple_of((b * PIECE + u) * sub, sub), sub)],
                    gsem.at[slot]).start()
            return c

        lax.fori_loop(0, nb, body, 0)

    def out_copies(t, act):
        base = tab[1, t]
        n = tab[2, t]
        full = n // PIECE

        def big(b, c):
            act(pltpu.make_async_copy(
                obuf.at[pl.ds(pl.multiple_of(b * PIECE * sub, PIECE * sub), PIECE * sub)],
                out.at[pl.ds(pl.multiple_of((base + b * PIECE) * sub, sub), PIECE * sub)], osem))
            return c

        def small(b, c):
            act(pltpu.make_async_copy(
                obuf.at[pl.ds(pl.multiple_of(b * sub, sub), sub)],
                out.at[pl.ds(pl.multiple_of((base + b) * sub, sub), sub)], osem))
            return c

        lax.fori_loop(0, full, big, 0)
        lax.fori_loop(full * PIECE, n, small, 0)

    @pl.when(i == 0)
    def _():
        fetch(0, 0)

    @pl.when(i + 1 < total)
    def _():
        fetch(i + 1, (i + 1) % 2)

    @pl.when(i < total)
    def _():
        slot = i % 2

        def wait(b, c):
            pltpu.make_async_copy(
                x_hbm.at[pl.ds(0, PIECE * sub)], xbuf.at[slot, pl.ds(0, PIECE * sub)], gsem.at[slot]).wait()
            return c

        lax.fori_loop(0, (tab[2, i] + PIECE - 1) // PIECE, wait, 0)

        def compute(m):
            relayout_in(xbuf.at[slot], xf, xb, m, sub)
            x = xb[:m, :]
            f = w1.shape[2]
            for c in range(0, f, COLS):
                hi = min(c + COLS, f)
                u = jnp.dot(x, w1[0, :, c:hi], preferred_element_type=jnp.float32)
                v = jnp.dot(x, w3[0, :, c:hi], preferred_element_type=jnp.float32)
                ab[:m, c:hi] = (u * jax.nn.sigmoid(u) * v).astype(jnp.bfloat16)
            a = ab[:m, :]
            for h in range(0, sub, OSUB):
                o = jnp.dot(a, w2[0, :, h * LANES:(h + OSUB) * LANES], preferred_element_type=jnp.float32)
                for j in range(OSUB):
                    xf[pl.ds(h + j, m, stride=sub), :] = o[:, j * LANES:(j + 1) * LANES]

            @pl.when(i > 0)
            def _():
                out_copies(i - 1, lambda c: c.wait())

            def narrow(b, c):
                r = pl.multiple_of(b * 32 * sub, 32 * sub)
                obuf[pl.ds(r, 32 * sub), :] = xf[pl.ds(r, 32 * sub), :].astype(jnp.bfloat16)
                return c

            lax.fori_loop(0, m // 32, narrow, 0)

        if TAIL:
            @pl.when(tab[2, i] > TAIL)
            def _():
                compute(TM)

            @pl.when(tab[2, i] <= TAIL)
            def _():
                compute(TAIL)
        else:
            compute(TM)
        out_copies(i, lambda c: c.start())

    @pl.when(jnp.logical_and(i == nt - 1, total > 0))
    def _():
        out_copies(total - 1, lambda c: c.wait())


def ffn(tab, tok, x3, w1, w3, w2, cap, base3=0):
    nt = tab.shape[1]
    d, f = w1.shape[1:]
    sub = d // LANES
    wspec = lambda shape, b=0: pl.BlockSpec((1,) + shape, lambda i, tab, tok: (tab[0, i] + b if b else tab[0, i], 0, 0))
    return pl.pallas_call(
        functools.partial(ffn_kernel, nt, sub),
        out_shape=jax.ShapeDtypeStruct((cap * sub, LANES), jnp.bfloat16),
        grid_spec=pltpu.PrefetchScalarGridSpec(
            num_scalar_prefetch=2,
            grid=(nt,),
            in_specs=[pl.BlockSpec(memory_space=pl.ANY), wspec((d, f)), wspec((d, f), base3), wspec((f, d))],
            out_specs=pl.BlockSpec(memory_space=pl.ANY),
            scratch_shapes=[
                pltpu.VMEM((2, TM * sub, LANES), jnp.bfloat16),
                pltpu.VMEM((TM * sub, LANES), jnp.float32),
                pltpu.VMEM((TM, d), jnp.bfloat16),
                pltpu.VMEM((TM, f), jnp.bfloat16),
                pltpu.VMEM((TM * sub, LANES), jnp.bfloat16),
                pltpu.SemaphoreType.DMA((2,)),
                pltpu.SemaphoreType.DMA,
            ]),
        compiler_params=pltpu.CompilerParams(
            dimension_semantics=("arbitrary",), vmem_limit_bytes=60 * 1024 * 1024),
        cost_estimate=pl.CostEstimate(flops=6 * cap * d * f, bytes_accessed=6 * 8 * d * f, transcendentals=cap * f),
        name="expert_ffn",
    )(tab, tok, x3, w1, w3, w2)


RB = 512


def combine_kernel(nbs, sub, first, final, meta, tok_ref, gate_ref, *refs):
    nsrc = len(nbs)
    srcs = refs[:nsrc]
    rest = refs[nsrc:]
    if not first:
        acc_in, rest = rest[0], rest[1:]
    out, acc, buf, xf, xb, sem, asem = rest[:7]
    td, _ = acc.shape
    steps = [(q, b) for q in range(nsrc) for b in range(nbs[q])]
    total = len(steps)
    i = pl.program_id(0)
    off = [sum(nbs[:q]) for q in range(nsrc)]
    rows = RB * sub

    def each_source(t, fn):
        for q in range(nsrc):
            @pl.when(jnp.logical_and(t >= off[q], t < off[q] + nbs[q]))
            def _(q=q):
                b = t - off[q]
                fn(srcs[q].at[pl.ds(pl.multiple_of(b * rows, rows), rows)])

    def live(t):
        return meta[t] > 0

    @pl.when(i == 0)
    def _():
        if first:
            acc[...] = jnp.zeros_like(acc)
        else:
            cp = pltpu.make_async_copy(acc_in, acc, asem)
            cp.start()

        @pl.when(live(0))
        def _():
            each_source(0, lambda r: pltpu.make_async_copy(r, buf.at[0], sem.at[0]).start())

        if not first:
            cp.wait()

    @pl.when(i + 1 < total)
    def _():
        @pl.when(live(i + 1))
        def _():
            each_source(i + 1, lambda r: pltpu.make_async_copy(r, buf.at[(i + 1) % 2], sem.at[(i + 1) % 2]).start())

    @pl.when(live(i))
    def _():
        pltpu.make_async_copy(srcs[0].at[pl.ds(0, rows)], buf.at[i % 2], sem.at[i % 2]).wait()
        relayout_in(buf.at[i % 2], xf, xb, RB, sub)
        n = meta[i]

        @pl.when(n < RB)
        def _():
            keep = lax.broadcasted_iota(jnp.int32, (RB, LANES), 0) < n
            for j in range(sub):
                cur = xb[:, j * LANES:(j + 1) * LANES].astype(jnp.float32)
                xb[:, j * LANES:(j + 1) * LANES] = jnp.where(keep, cur, 0.0).astype(jnp.bfloat16)

        tb = 256

        def tokens(c, z):
            r = pl.multiple_of(c * tb, tb)
            ids = lax.broadcasted_iota(jnp.int32, (tb, RB), 0) + r
            g = jnp.where(ids == tok_ref[0], gate_ref[0], 0.0).astype(jnp.bfloat16)
            acc[pl.ds(r, tb), :] += jnp.dot(g, xb[...], preferred_element_type=jnp.float32)
            return z

        lax.fori_loop(0, td // tb, tokens, 0)

    @pl.when(i == total - 1)
    def _():
        if final:
            ob = rest[7]
            cb = 256
            for c in range(td // cb):
                if c >= 2:
                    pltpu.make_async_copy(ob.at[c % 2], out.at[pl.ds((c - 2) * cb, cb)], sem.at[c % 2]).wait()
                ob[c % 2] = acc[c * cb:(c + 1) * cb, :].astype(jnp.bfloat16)
                pltpu.make_async_copy(ob.at[c % 2], out.at[pl.ds(c * cb, cb)], sem.at[c % 2]).start()
            for c in (td // cb - 2, td // cb - 1):
                pltpu.make_async_copy(ob.at[c % 2], out.at[pl.ds(c * cb, cb)], sem.at[c % 2]).wait()
        else:
            cp = pltpu.make_async_copy(acc, out, asem)
            cp.start()
            cp.wait()


def combine(acc, srcs, toks, gates, lens, td, d, final):
    sub = d // LANES
    nbs = [s.shape[0] // (RB * sub) for s in srcs]
    first = acc is None
    meta = jnp.concatenate([jnp.clip(n - jnp.arange(nb, dtype=jnp.int32) * RB, 0, RB) for n, nb in zip(lens, nbs)])
    total = sum(nbs)
    tokv = jnp.concatenate(toks).reshape(total, 1, RB)
    gatev = jnp.concatenate(gates).reshape(total, 1, RB)
    vspec = pl.BlockSpec((1, 1, RB), lambda i, m: (i, 0, 0))
    scratch = [
        pltpu.VMEM((td, d), jnp.float32),
        pltpu.VMEM((2, RB * sub, LANES), jnp.bfloat16),
        pltpu.VMEM((RB * sub, LANES), jnp.float32),
        pltpu.VMEM((RB, d), jnp.bfloat16),
        pltpu.SemaphoreType.DMA((2,)),
        pltpu.SemaphoreType.DMA,
    ]
    if final:
        scratch.append(pltpu.VMEM((2, 256, d), jnp.bfloat16))
    extra = [] if first else [acc]
    return pl.pallas_call(
        functools.partial(combine_kernel, nbs, sub, first, final),
        out_shape=jax.ShapeDtypeStruct((td, d), jnp.bfloat16 if final else jnp.float32),
        grid_spec=pltpu.PrefetchScalarGridSpec(
            num_scalar_prefetch=1,
            grid=(total,),
            in_specs=[vspec, vspec] + [pl.BlockSpec(memory_space=pl.ANY)] * (len(srcs) + len(extra)),
            out_specs=pl.BlockSpec(memory_space=pl.ANY),
            scratch_shapes=scratch),
        compiler_params=pltpu.CompilerParams(
            dimension_semantics=("arbitrary",), vmem_limit_bytes=48 * 1024 * 1024),
        cost_estimate=pl.CostEstimate(flops=2 * total * RB * td * d, bytes_accessed=total * RB * d * 2, transcendentals=0),
        name="combine",
    )(meta, tokv, gatev, *srcs, *extra)


def plan(ridx, gates, ep, loc):
    td, k = ridx.shape
    n = td * k
    ne = ep * loc
    nb = n // BLK
    e = ridx.reshape(nb, BLK)
    oh = e[:, :, None] == jnp.arange(ne, dtype=jnp.int32)
    ohb = oh.astype(jnp.bfloat16)
    tri = (jnp.arange(BLK)[:, None] > jnp.arange(BLK)[None, :]).astype(jnp.bfloat16)
    inb = jnp.einsum("ij,bjg->big", tri, ohb, preferred_element_type=jnp.float32)
    tot = jnp.sum(ohb.astype(jnp.float32), axis=1)
    low = (jnp.arange(nb)[:, None] > jnp.arange(nb)[None, :]).astype(jnp.bfloat16)
    before = jnp.dot(low, tot.astype(jnp.bfloat16), preferred_element_type=jnp.float32)
    cnt = (before[-1] + tot[-1]).astype(jnp.int32)
    cold = cnt.at[0].set(0)
    starts = prefix(cold) - cold
    off = starts.at[0].set(n - cnt[0]).astype(jnp.float32)
    pos = jnp.sum(jnp.where(oh, inb + (before + off)[:, None, :], 0.0), axis=2).astype(jnp.int32).reshape(n)
    hi = (pos[:, None] // BLK == jnp.arange(nb, dtype=jnp.int32)).astype(jnp.bfloat16)
    lo = pos[:, None] % BLK == jnp.arange(BLK, dtype=jnp.int32)
    t = jnp.arange(n, dtype=jnp.int32) // k
    vals = [(t // BLK).astype(jnp.bfloat16), (t % BLK).astype(jnp.bfloat16), gates.reshape(n)]
    rhs = jnp.concatenate([jnp.where(lo, v[:, None], jnp.zeros((), jnp.bfloat16)) for v in vals], axis=1)
    m = jnp.einsum("nh,nl->hl", hi, rhs, preferred_element_type=jnp.float32)
    tok = (m[:, :BLK] * BLK + m[:, BLK:2 * BLK]).astype(jnp.int32).reshape(n)
    return tok, m[:, 2 * BLK:].reshape(n), starts.reshape(ep, loc), cold.reshape(ep, loc), cnt[0]


def prefix(v):
    m = v.shape[-1]
    upto = jnp.arange(m)[:, None] <= jnp.arange(m)[None, :]
    return jnp.sum(jnp.where(upto, v[..., :, None], 0), axis=-2)


def tile_tables(counts, nt):
    ep, ns = counts.shape
    tiles = (counts + TM - 1) // TM
    tend = prefix(tiles)
    rstart = prefix(counts) - counts
    total = tend[:, -1:]
    slot = jnp.arange(ns, dtype=jnp.int32)[None, :]
    i = jnp.arange(nt, dtype=jnp.int32)[None, :]
    ic = jnp.minimum(i, jnp.maximum(total - 1, 0))
    sel = jnp.sum((ic[:, :, None] >= tend[:, None, :]).astype(jnp.int32), axis=2)
    one = sel[:, :, None] == slot[:, None, :]
    pick = lambda v: jnp.sum(jnp.where(one, v[:, None, :], 0), axis=2)
    within = (ic - pick(tend - tiles)) * TM
    rows = jnp.where(i < total, jnp.minimum(pick(counts) - within, TM), 0)
    tab = jnp.stack([sel, pick(rstart) + within, rows, jnp.broadcast_to(total, (ep, nt))], axis=1)
    return tab.astype(jnp.int32)


def solution(mesh):
    p = mesh.shape["ep"]

    def layer(x, ridx, gates, w1, w3, w2):
        td, d = x.shape
        k = ridx.shape[1]
        loc = w1.shape[0] - 1
        sub = d // LANES
        n = td * k
        cap = n // p
        me = lax.axis_index("ep")

        def swap(v, b):
            return lax.ppermute(v, "ep", [(q, q ^ b) for q in range(p)])

        nt = cap // TM + loc
        tok, gate, starts, groups, nhot = plan(ridx, gates, p, loc)
        tabs = tile_tables(groups, nt)
        recs = jnp.concatenate([starts[:, :1], tabs.reshape(p, 4 * nt)], axis=1)
        recs = jnp.pad(recs, ((0, 0), (0, LANES - recs.shape[1])))
        pad = td + LANES
        tokp = jnp.concatenate([tok, jnp.zeros((pad,), jnp.int32)])
        every = lax.all_gather(jnp.concatenate([tokp, recs.reshape(-1)]), "ep")

        x3 = x.reshape(td * sub, LANES)
        blk = {0: x3, 1: swap(x3, 1)}
        x3, every = lax.optimization_barrier((x3, every))
        blk[2] = swap(x3, 2)
        blk[4] = swap(x3, 4)
        blk[3] = swap(blk[2], 1)
        blk[6] = swap(blk[2], 4)
        blk[5] = swap(blk[4], 1)
        blk[7] = swap(blk[6], 1)

        holder = me % 4 < 2
        hslot = jnp.where(me == 0, 0, loc)
        take = lambda w: lax.dynamic_slice_in_dim(w, hslot, 1, axis=0)
        own = [jnp.concatenate([take(w1), take(w3)], axis=0), take(w2)]
        own[0], own[1], blk[2] = lax.optimization_barrier((own[0], own[1], blk[2]))
        far, twin = [], []
        for i, v in enumerate(own):
            far.append(lax.ppermute(v, "ep", [(q, q + 2) for q in range(0, p, 4)]))
            twin.append(lax.ppermute(far[i], "ep", [(q, q + 1) for q in range(2, p, 4)]))

        rec = lax.dynamic_slice_in_dim(every, n + pad + me * LANES, LANES, axis=1)
        dev = jnp.arange(p, dtype=jnp.int32)
        rel = (me ^ dev)[:, None] == dev[None, :]
        rec = jnp.sum(jnp.where(rel[:, :, None], rec[None, :, :], 0), axis=1)
        gatep = jnp.concatenate([gate, jnp.zeros((pad,), jnp.float32)])
        per = jnp.sum(groups, axis=1)
        outs, toks, gts, lens = {}, {}, {}, {}
        prev = None
        for j in ORDER:
            if j == HOT:
                nth = td // TM
                left = nhot - jnp.arange(nth, dtype=jnp.int32) * TM
                total = (nhot + TM - 1) // TM
                tab = jnp.stack([jnp.zeros_like(left), jnp.arange(nth, dtype=jnp.int32) * TM,
                                 jnp.clip(left, 0, TM), jnp.broadcast_to(total, (nth,))])
                seg = lax.dynamic_slice_in_dim(tokp, n - nhot, td + PIECE)
                h = [jnp.where(holder, o, jnp.where(me % 2 == 0, a, b)) for o, a, b in zip(own, far, twin)]
            else:
                tab = rec[j, 1:1 + 4 * nt].reshape(4, nt)
                seg = lax.dynamic_slice(every, (me ^ j, rec[j, 0]), (1, cap + PIECE)).reshape(cap + PIECE)
            if prev is not None:
                tab, outs[prev] = lax.optimization_barrier((tab, outs[prev]))
                if prev not in (0, HOT):
                    outs[prev] = swap(outs[prev], prev)
            if j == HOT:
                outs[j] = ffn(tab, seg, blk[0], h[0], h[0], h[1], td, 1)
                mine, rows = n - nhot, td
                lens[j] = nhot
            else:
                outs[j] = ffn(tab, seg, blk[j], w1, w3, w2, cap)
                mine, rows = lax.dynamic_index_in_dim(starts[:, 0], me ^ j, 0, keepdims=False), cap
                lens[j] = lax.dynamic_index_in_dim(per, me ^ j, 0, keepdims=False)
            toks[j] = lax.dynamic_slice_in_dim(tokp, mine, rows)
            gts[j] = lax.dynamic_slice_in_dim(gatep, mine, rows)
            prev = j
        if prev not in (0, HOT):
            outs[prev] = swap(outs[prev], prev)
        acc = None
        for part in PARTS:
            pick = lambda m: [m[j] for j in part]
            acc = combine(acc, pick(outs), pick(toks), pick(gts), pick(lens), td, d, part is PARTS[-1])
        return acc

    spec_t = P(("dp", "ep"), None)
    spec_w = P("ep", None, None)
    return jax.shard_map(layer, mesh=mesh, in_specs=(spec_t, spec_t, spec_t, spec_w, spec_w, spec_w), out_specs=spec_t, check_vma=False)
```
